32 devices in a mesh: dx: 4 (over x, core), dy: 8 (over z, y).
Axes of the slice: x: 2, y: 2, z: 4, core: 2. Of those that a mesh axis runs over, the one named last changes fastest.
Arguments:
- positions: float32 [3, 65536], P(None, ('dx', 'dy')), may hold values from -6 to 6
- masses: float32 [65536], P(('dx', 'dy')), may hold values from 0.003 to 0.03
- centers: float32 [3, 32768], P(None, ('dx', 'dy')), may hold values from -3 to 3
- radii: float32 [32768], P(('dx', 'dy')), may hold values from 0.6 to 1.8
- pair_block: int32 [16384], P(('dx', 'dy')), may hold values from 0 to 15
- pair_halo: int32 [16384], P(('dx', 'dy')), may hold values from -1 to 1023, as said below
Outputs:
- centers_out: float32 [3, 32768], P(None, ('dx', 'dy'))
- radii_out: float32 [32768], P(('dx', 'dy'))
- profile: float32 [16, 32768], P(None, ('dx', 'dy'))
The draws below stay inside these ranges and needn't reach their ends.
Inputs may be any that keep to these rules, and one draw needn't show every extreme that they name: `pair_halo`: for each domain and each owner, the 16 slots hold the live halo indices first and then -1; in every draw some owner receives 16 live slots from every domain.
All inputs are finite; a program needn't handle non-finite values.
Results may differ from the reference program's by a relative error of at most 0.0003.
Values sent between devices are 32-bit elements; how exact they have to be, the bound alone decides.
A program may use at most 64 MiB of HBM per device.

```python
import math
import jax
import jax.numpy as jnp
from jax import lax

SHELLS = 16
BLOCK = 128
ITERS = 2
BLOCKS_DEV = 16
CAP = 16
HALO_DEV = 1024
HALOS = 32768
PARTICLES = 65536
PAIRS = 16384
DEVICES = 32


def draw_pair_halo(key, part):
    key_heavy = jax.random.fold_in(key, 11)
    key_light = jax.random.fold_in(key, 12)
    key_column = jax.random.fold_in(key, 13)
    key_index = jax.random.fold_in(key, 14)
    heavy = jax.random.randint(key_heavy, (DEVICES, 1), 0, 4) == 0
    light = jax.random.randint(key_light, (DEVICES, DEVICES), 0, CAP // 2 + 1)
    column = jax.random.randint(key_column, (), 0, DEVICES)
    full = heavy | (jnp.arange(DEVICES)[None, :] == column)
    live = jnp.where(full, CAP, light)
    halos = jax.random.randint(key_index, (DEVICES, DEVICES, CAP), 0, HALO_DEV)
    slot = jnp.arange(CAP)[None, None, :]
    return jnp.where(slot < live[:, :, None], halos, -1).reshape(-1).astype(jnp.int32)


def set_ends(array, key, smallest, top_value):
    longest = array.shape.index(max(array.shape))
    spots = []
    for shift in (0, 1):
        where = [jax.random.randint(jax.random.fold_in(key, axis), (), 0, length) for axis, length in enumerate(array.shape)]
        where[longest] = (where[longest] + shift) % array.shape[longest]
        spots.append(tuple(where))
    return array.at[spots[0]].set(smallest).at[spots[1]].set(top_value)


def levels(rng, shape, pieces, least, high):
    def one(dim, parts):
        steps = jax.random.uniform(jax.random.fold_in(jax.random.fold_in(rng, 6), dim), (parts,), jnp.float32, least / len(pieces), high / len(pieces))
        return jnp.repeat(jnp.exp(steps), shape[dim] // parts).reshape((-1,) + (1,) * (len(shape) - dim - 1))

    level = one(*pieces[0])
    for cut in pieces[1:]:
        level = level * one(*cut)
    return level


def scatter_about(rng, dims, deviation, limit, pieces=(), kind=jnp.bfloat16):
    factor_of = levels(rng, dims, pieces, -0.22, 0.18) if pieces else 1.0
    drawn = jax.random.normal(rng, dims, jnp.float32) * deviation * factor_of
    return jnp.minimum(jnp.maximum(drawn, -limit), limit).astype(kind)


def setup_inputs(seed: int = 0) -> dict:
    streams_of = jax.random.split(jax.random.key(seed), 7)
    positions = scatter_about(streams_of[0], (3, PARTICLES), 1.0, 6.0, ((1, 32),), jnp.float32)
    masses = jnp.clip(jnp.exp(math.log(0.03) - 2.3025851 * jax.random.uniform(streams_of[1], (PARTICLES,), jnp.float32) ** levels(streams_of[1], (PARTICLES,), ((0, 32),), -0.2, 0.2)), 0.003, 0.03)
    centers = scatter_about(streams_of[2], (3, HALOS), 0.3, 3.0, ((1, 32),), jnp.float32)
    radii = jnp.clip(jnp.exp(math.log(1.8) - 1.0986122 * jax.random.uniform(streams_of[3], (HALOS,), jnp.float32) ** levels(streams_of[3], (HALOS,), ((0, 32),), -0.2, 0.2)), 0.6, 1.8)
    pair_block = set_ends(jax.random.randint(streams_of[4], (PAIRS,), 0, BLOCKS_DEV), jax.random.fold_in(streams_of[4], 1), 0, BLOCKS_DEV - 1).astype(jnp.int32)
    pair_halo = draw_pair_halo(jax.random.fold_in(streams_of[6], 71), 0)
    return {"positions": positions, "masses": masses, "centers": centers, "radii": radii, "pair_block": pair_block, "pair_halo": pair_halo}


def slot_terms(points, weights, center, radius, live):
    offset = points - center[:, :, None]
    dist = jnp.sqrt(lax.optimization_barrier(jnp.sum(offset * offset, axis=0)))
    scaled = dist * (SHELLS / 2.0 / radius)[:, None]
    middles = jnp.arange(SHELLS, dtype=jnp.float32) + 0.5
    tent = jnp.maximum(0.0, 1.0 - jnp.abs(scaled[None] - middles[:, None, None]))
    massed = weights * live[:, None]
    shells = lax.optimization_barrier(jnp.sum(tent * massed[None], axis=2))
    inner = jnp.clip(SHELLS / 2.0 - scaled, 0.0, 1.0) * massed
    total = lax.optimization_barrier(jnp.sum(inner, axis=1))
    moment = lax.optimization_barrier(jnp.sum(offset * inner[None], axis=2))
    return jnp.concatenate([shells, total[None], moment], axis=0)

def advance(centers, radii, sums):
    profile = jnp.cumsum(sums[:SHELLS], axis=0)
    enclosed = profile[SHELLS // 2 - 1]
    ratio = (1.0 + enclosed) / (1.0 + radii * radii * radii)
    new_radii = radii * ratio ** (1.0 / 3.0)
    new_centers = centers + sums[SHELLS + 1:] / jnp.maximum(sums[SHELLS], 1.0)
    return (new_centers, new_radii, profile)

def reference(positions, masses, centers, radii, pair_block, pair_halo):
    points = positions.reshape(3, DEVICES, BLOCKS_DEV, BLOCK)
    weights = masses.reshape(DEVICES, BLOCKS_DEV, BLOCK)
    blocks = pair_block.reshape(DEVICES, DEVICES * CAP)
    halos = pair_halo.reshape(DEVICES, DEVICES, CAP)
    owners = jnp.arange(DEVICES, dtype=jnp.int32)[None, :, None] * HALO_DEV
    target = jnp.where(halos >= 0, halos + owners, HALOS).reshape(DEVICES, DEVICES * CAP).astype(jnp.int32)
    profile = None
    for step in range(ITERS):

        def source(total, index):
            mine = lax.dynamic_index_in_dim(blocks, index, 0, keepdims=False)
            pts = jnp.take(lax.dynamic_index_in_dim(points, index, 1, keepdims=False), mine, axis=1)
            wts = jnp.take(lax.dynamic_index_in_dim(weights, index, 0, keepdims=False), mine, axis=0)
            dest = lax.dynamic_index_in_dim(target, index, 0, keepdims=False)
            safe = jnp.minimum(dest, HALOS - 1)
            live = (dest < HALOS).astype(jnp.float32)
            terms = slot_terms(pts, wts, jnp.take(centers, safe, axis=1), jnp.take(radii, safe), live)
            return (total + jax.ops.segment_sum(terms.T, dest, num_segments=HALOS + 1), None)
        start = jnp.zeros((HALOS + 1, SHELLS + 4), jnp.float32)
        sums, _ = lax.scan(source, start, jnp.arange(DEVICES, dtype=jnp.int32))
        centers, radii, profile = advance(centers, radii, sums[:HALOS].T)
    return (centers, radii, profile)
```

```python
import functools

import jax
import jax.numpy as jnp
from jax import lax
from jax.experimental import pallas as pl
from jax.experimental.pallas import tpu as pltpu
from jax.sharding import PartitionSpec as P

SHELLS = 16
BLOCK = 128
ITERS = 2
GROUP = 8
ROWS = 32
CHUNK = 32
HUB = 0


def split3(value):
    high = value.astype(jnp.bfloat16)
    rest = value - high.astype(jnp.float32)
    middle = rest.astype(jnp.bfloat16)
    low = (rest - middle.astype(jnp.float32)).astype(jnp.bfloat16)
    return jnp.concatenate([high, middle, low], axis=0)


def join3(value):
    rows = value.shape[0] // 3
    return value[:rows] + (value[rows : 2 * rows] + value[2 * rows :])


def kernel(
    sizes,
    pos, mass, cen, rad, blocks, halos,
    cen_out, rad_out, prof_out,
    raw_pos, raw_mass, raw_pair, data, pick, points, onehot, terms, state, asked,
    local_sem, send_sem, recv_sem, ready,
):
    ndx, ndy, slots, count = sizes
    n = ndx * ndy
    half = n // 2
    groups = n // GROUP
    halo_dev = rad.shape[1]
    mx = lax.axis_index("dx")
    my = lax.axis_index("dy")
    me = mx * ndy + my
    core = lax.rem(mx, 2)
    size_a, size_b, size_c = ndx // 2, 2, ndy // 2
    MESH = pl.DeviceIdType.MESH

    def flip(value, step, size):
        if size & (size - 1):
            return lax.rem(value + step, size)
        bit = 1
        while bit < size:
            if step & bit:
                value = value + bit * (1 - 2 * lax.rem(value // bit, 2))
            bit *= 2
        return value

    def at_step(step3, step2, step1):
        a, b, c = mx // 2, lax.rem(my, 2), my // 2
        c = flip(c, step1, size_c)
        if size_a == size_b:
            a0, b0 = flip(a, step3, size_a), flip(b, step2, size_b)
            a1, b1 = flip(a, step2, size_a), flip(b, step3, size_b)
            a, b = a0 + core * (a1 - a0), b0 + core * (b1 - b0)
        else:
            a, b = flip(a, step3, size_a), flip(b, step2, size_b)
        return 2 * a + core, 2 * c + b

    sibling = (mx + 1 - 2 * core, my)
    row_me = (me * slots) // 128
    pair_rows = raw_pair.shape[1]

    def label(p3, p2, p1):
        return (p3 * size_b + p2) * size_c + p1

    line = list(range(size_c))
    plane = [(p3, p2) for p3 in range(size_a) for p2 in range(size_b) if p3 or p2]
    plane.sort(key=lambda p: -(p[0] > 0) - (p[1] > 0))

    rank = []
    for p1 in line:
        rank.append((0, p1, 0, label(0, 0, p1)))
        rank.append((0, p1, 1, label(0, 0, p1) + half))
        for p3, p2 in plane:
            rank.append((1, p1, 0, label(p3, p2, p1)))
            rank.append((1, p1, 1, label(p3, p2, p1) + half))
    rank.sort()
    place_of = {t: i for i, (_, _, _, t) in enumerate(rank)}

    kinds = (None, data)
    first = jnp.logical_and(mx // 2 == 0, my == 0)
    hub = half <= HUB

    def coords(p3, p2):
        if size_a == size_b:
            return p3 + core * (p2 - p3), p2 + core * (p3 - p2)
        return p3, p2

    def inward(p3, p2, p1):
        a, b = coords(p3, p2)
        far = (mx // 2 - a) * (mx // 2 - a) + (lax.rem(my, 2) - b) * (lax.rem(my, 2) - b)
        return far + (my // 2 - p1) * (my // 2 - p1) == 0

    def copy(kind, source, target, device):
        u = kind * n
        return pltpu.make_async_remote_copy(
            src_ref=kinds[kind].at[place_of[source]], dst_ref=kinds[kind].at[place_of[target]],
            send_sem=send_sem.at[u + target], recv_sem=recv_sem.at[u + target],
            device_id=device, device_id_type=MESH,
        )

    sent = []

    def launch(kind, source, target, device, go=None):
        one = copy(kind, source, target, device)
        if go is None:
            one.start()
        else:
            pl.when(go)(one.start)
        sent.append((one, go))

    zed = my // 2
    spot = (mx // 2) * size_b + lax.rem(my, 2)

    def outer_line(step):
        return flip(zed, step, size_c) > zed

    def outer_plane(p3, p2):
        tx, ty = at_step(p3, p2, 0)
        return (tx // 2) * size_b + lax.rem(ty, 2) > spot

    peers = [(0, 0, step) for step in line[1:]] + [(p3, p2, 0) for p3, p2 in plane]
    peers.sort(key=lambda p: (p[0] > 0) + (p[1] > 0) + p[2])

    def outer(peer):
        return outer_line(peer[2]) if peer[2] else outer_plane(peer[0], peer[1])

    def relay(kind, t):
        p1 = t % size_c
        if 0 < t < size_c:
            for p3, p2 in plane:
                go = jnp.logical_not(inward(p3, p2, 0)) if hub else None
                launch(kind, t, label(p3, p2, p1), at_step(p3, p2, 0), go)
        if t < half:
            launch(kind, t, t + half, sibling)

    def begin(kind):
        if hub:
            for p3, p2 in plane:
                for step in line[1:]:
                    launch(kind, 0, label(p3, p2, step), at_step(p3, p2, step), inward(p3, p2, step))
        for peer in reversed(peers):
            go = jnp.logical_not(outer(peer))
            launch(kind, 0, label(*peer), at_step(*peer), go)

        @pl.when(core == 0)
        def _():
            pl.semaphore_wait(ready.at[0], 1)

        relay(kind, 0)
        for peer in peers:
            go = outer(peer)

            @pl.when(go)
            def _(peer=peer):
                pl.semaphore_wait(ready.at[label(*peer)], 1)

            launch(kind, 0, label(*peer), at_step(*peer), go)

    def arrive(kind, t):
        copy(kind, 0, t, sibling).wait_recv()
        relay(kind, t)

    own = [
        pltpu.make_async_copy(pos, raw_pos, local_sem.at[0]),
        pltpu.make_async_copy(mass, raw_mass, local_sem.at[1]),
        pltpu.make_async_copy(blocks, raw_pair.at[0], local_sem.at[2]),
        pltpu.make_async_copy(halos, raw_pair.at[1], local_sem.at[3]),
        pltpu.make_async_copy(cen, cen_out, local_sem.at[4]),
        pltpu.make_async_copy(rad, rad_out, local_sem.at[5]),
    ]
    barrier = pltpu.get_barrier_semaphore()

    def greet(device):
        pl.semaphore_signal(barrier, inc=1, device_id=device, device_id_type=MESH)

    def answer(t, device):
        pl.semaphore_signal(ready.at[t], inc=1, device_id=device, device_id_type=MESH)

    for one in own:
        one.start()
    for peer in peers:
        pl.when(outer(peer))(functools.partial(greet, at_step(*peer)))
    pl.when(core == 0)(functools.partial(greet, sibling))
    extra = 0
    if hub:

        @pl.when(first)
        def _():
            for p3, p2 in plane:
                for step in line[1:]:
                    greet(at_step(p3, p2, step))

        off = jnp.minimum(spot, 1)
        extra = off * jnp.minimum(zed, 1)
    lower = zed + spot + core + extra

    @pl.when(lower > 0)
    def _():
        pl.semaphore_wait(barrier, lower)

    for peer in peers:
        pl.when(jnp.logical_not(outer(peer)))(functools.partial(answer, label(*peer), at_step(*peer)))
    pl.when(core == 1)(functools.partial(answer, 0, sibling))
    for one in own:
        one.wait()
    mine = place_of[0]
    for b in range(count):
        part = raw_pos[:, b * BLOCK : (b + 1) * BLOCK]
        for i in range(3):
            data[mine, i * count + b : i * count + b + 1, :] = part[i : i + 1]
    data[mine, 3 * count : 4 * count, :] = raw_mass[...]
    for i in range(2):
        at = 4 * count + i * pair_rows
        data[mine, at : at + pair_rows, :] = raw_pair[i].astype(jnp.float32)
    state[...] = jnp.zeros_like(state)
    terms[...] = jnp.zeros_like(terms)
    state[0:3, :] = cen_out[...]
    state[3:4, :] = rad_out[...]
    begin(1)

    lane0 = me * slots - row_me * 128
    lanes = lax.broadcasted_iota(jnp.int32, (GROUP, halo_dev), 1).astype(jnp.float32)
    spots = lax.broadcasted_iota(jnp.int32, (GROUP, GROUP * count), 1).astype(jnp.float32)
    place = lax.broadcasted_iota(jnp.int32, (GROUP, 128), 0).astype(jnp.float32)
    shift = lax.rem(128 - lane0, 128)

    def prepare(g):
        lo = g * GROUP * slots
        if not isinstance(g, int):
            lo = pl.multiple_of(lo, GROUP * slots)

        def taken(i):
            at = 4 * count + i * pair_rows + row_me
            part = data[pl.ds(g * GROUP, GROUP), pl.ds(at, 1), :].reshape(GROUP, 128)
            return pltpu.roll(part, shift, 1)

        rows = taken(1)
        want = taken(0) + place * float(count)
        for j in range(0, slots, 2):
            start = lo + j * GROUP
            for values, iota, out in ((rows, lanes, onehot), (want, spots, pick)):
                pair = [
                    jnp.where(values[:, i : i + 1] == iota, 1.0, 0.0) for i in (j, j + 1)
                ]
                both = jnp.concatenate(pair, axis=0).astype(jnp.bfloat16)
                out[pl.ds(start, 2 * GROUP), :] = both
        asked[:, pl.ds(lo, GROUP * slots)] = join3(
            lax.dot_general(
                split3(state[...]), onehot[pl.ds(lo, GROUP * slots), :], (((1,), (1,)), ((), ())),
                preferred_element_type=jnp.float32,
            )
        )

    def ask():
        asked[...] = join3(
            lax.dot_general(
                split3(state[...]), onehot[...], (((1,), (1,)), ((), ())),
                preferred_element_type=jnp.float32,
            )
        )

    width = GROUP * slots

    def evaluate(g):
        lo = pl.multiple_of(g * width, width)
        mine = asked[0:4, pl.ds(lo, width)]
        cx, cy, cz, radius = (mine[i : i + 1] for i in range(4))
        scale = (SHELLS / 2.0) / jnp.where(radius > 0.0, radius, 1.0)

        def fold(value):
            return jnp.sum(value.reshape(CHUNK // 8, 8, width), axis=0)

        def chunk(c, acc):
            at = pl.ds(pl.multiple_of(c * CHUNK, CHUNK), CHUNK)
            ox = points[g, 0, at] - cx
            oy = points[g, 1, at] - cy
            oz = points[g, 2, at] - cz
            m = points[g, 3, at]
            u = jnp.sqrt(ox * ox + oy * oy + oz * oz) * scale
            top = m * jnp.minimum(u + 0.5, 1.0)
            ramp = m * (1.5 - u)
            out = []
            for k in range(SHELLS):
                out.append(acc[k] + fold(jnp.maximum(jnp.minimum(top, ramp), 0.0)))
                ramp = ramp + m
            inner = m * jnp.clip(SHELLS / 2.0 - u, 0.0, 1.0)
            out.append(acc[SHELLS] + fold(inner))
            for i, o in enumerate((ox, oy, oz)):
                out.append(acc[SHELLS + 1 + i] + fold(o * inner))
            return tuple(out)

        zero = jnp.zeros((8, width), jnp.float32)
        acc = lax.fori_loop(0, BLOCK // CHUNK, chunk, (zero,) * (SHELLS + 4))
        for k in range(SHELLS + 4):
            terms[k : k + 1, pl.ds(lo, width)] = jnp.sum(acc[k], axis=0, keepdims=True)

    def choose(g):
        chosen = pick[pl.ds(pl.multiple_of(g * width, width), width), :]
        for i in range(4):
            flat = data[pl.ds(g * GROUP, GROUP), i * count : (i + 1) * count, :]
            flat = flat.reshape(GROUP * count, BLOCK).T
            points[g, i] = join3(
                lax.dot_general(
                    split3(flat), chosen, (((1,), (1,)), ((), ())),
                    preferred_element_type=jnp.float32,
                )
            )

    def compute(g):
        choose(g)
        evaluate(g)

    def again(g, _):
        evaluate(g)
        return 0

    def advance():
        sums = join3(
            lax.dot_general(
                split3(terms[...]), onehot[...], (((1,), (0,)), ((), ())),
                preferred_element_type=jnp.float32,
            )
        )
        radius = state[3:4, :]
        enclosed = sums[SHELLS // 2 - 1 : SHELLS // 2]
        ratio = (1.0 + enclosed) / (1.0 + radius * radius * radius)
        state[3:4, :] = radius * jnp.exp(jnp.log(ratio) * (1.0 / 3.0))
        total = jnp.maximum(sums[SHELLS : SHELLS + 1], 1.0)
        state[0:3, :] = state[0:3, :] + sums[SHELLS + 1 : SHELLS + 4] / total
        return sums

    split = kinds[0] is not None

    def both(t):
        if split:
            arrive(0, t)
        arrive(1, t)

    if split:
        for t in line[1:]:
            arrive(0, t)
    for t in line[1:]:
        arrive(1, t)
    level = [rank[i][1] if rank[i][0] else -1 for i in range(n)]
    done = 0
    for p1 in line:
        for p3, p2 in reversed(plane):
            both(label(p3, p2, p1))
        while done < groups and (p1 == line[-1] or level[(done + 1) * GROUP - 1] < p1):
            for i in range(done * GROUP, (done + 1) * GROUP):
                if rank[i][3] >= half:
                    both(rank[i][3])
            prepare(done)
            compute(done)
            done += 1
    sums = advance()
    for step in range(1, ITERS):
        ask()
        lax.fori_loop(0, groups, again, 0)
        sums = advance()
    cen_out[...] = state[0:3, :]
    rad_out[...] = state[3:4, :]
    prof_out[...] = sums[:SHELLS]
    for one, go in sent:
        if go is None:
            one.wait_send()
        else:
            pl.when(go)(one.wait_send)


def hand(a, b, c, x, y, z, sem):
    copies = [
        pltpu.make_async_copy(source, target, sem.at[i])
        for i, (source, target) in enumerate(((a, x), (b, y), (c, z)))
    ]
    for copy in copies:
        copy.start()
    for copy in copies:
        copy.wait()


def body(positions, masses, centers, radii, pair_block, pair_halo):
    ndx = lax.axis_size("dx")
    ndy = lax.axis_size("dy")
    n = ndx * ndy
    halo_dev = radii.shape[0]
    count = masses.shape[0] // BLOCK
    slots = pair_halo.shape[0] // n
    total = n * slots
    groups = n // GROUP
    any_ref = pl.BlockSpec(memory_space=pl.ANY)
    vmem = pl.BlockSpec(memory_space=pltpu.VMEM)
    f32 = jnp.float32
    dma = pltpu.SemaphoreType.DMA
    out = pl.pallas_call(
        functools.partial(kernel, (ndx, ndy, slots, count)),
        out_shape=(
            pltpu.VMEM((3, halo_dev), f32),
            pltpu.VMEM((1, halo_dev), f32),
            pltpu.VMEM((SHELLS, halo_dev), f32),
        ),
        in_specs=[any_ref] * 6,
        out_specs=(vmem,) * 3,
        scratch_shapes=[
            pltpu.VMEM((3, count * BLOCK), f32),
            pltpu.VMEM((count, BLOCK), f32),
            pltpu.VMEM((2, total // 128, 128), jnp.int32),
            pltpu.VMEM((n, 4 * count + 2 * (total // 128), BLOCK), f32),
            pltpu.VMEM((total, GROUP * count), jnp.bfloat16),
            pltpu.VMEM((groups, 4, BLOCK, GROUP * slots), f32),
            pltpu.VMEM((total, halo_dev), jnp.bfloat16),
            pltpu.VMEM((ROWS, total), f32),
            pltpu.VMEM((16, halo_dev), f32),
            pltpu.VMEM((16, total), f32),
            dma((6,)),
            dma((2 * n,)),
            dma((2 * n,)),
            pltpu.SemaphoreType.REGULAR((n // 2,)),
        ],
        compiler_params=pltpu.CompilerParams(collective_id=0, has_side_effects=True),
    )(
        positions,
        masses.reshape(count, BLOCK),
        centers,
        radii.reshape(1, halo_dev),
        pair_block.reshape(total // 128, 128),
        pair_halo.reshape(total // 128, 128),
    )
    out = [pltpu.with_memory_space_constraint(x, pltpu.VMEM) for x in out]
    out = pl.pallas_call(
        hand,
        out_shape=tuple(jax.ShapeDtypeStruct(x.shape, f32) for x in out),
        in_specs=[vmem] * 3,
        out_specs=(any_ref,) * 3,
        scratch_shapes=[dma((3,))],
    )(*out)
    return out[0], out[1].reshape(halo_dev), out[2]


def solution(mesh):
    flat = P(("dx", "dy"))
    rows = P(None, ("dx", "dy"))
    in_specs = (rows, flat, rows, flat, flat, flat)
    out_specs = (rows, flat, rows)
    return jax.shard_map(body, mesh=mesh, in_specs=in_specs, out_specs=out_specs, check_vma=False)
```

```python
import functools

import jax
import jax.numpy as jnp
from jax import lax
from jax.experimental import pallas as pl
from jax.experimental.pallas import tpu as pltpu
from jax.sharding import PartitionSpec as P

SHELLS = 16
BLOCK = 128
ITERS = 2
GROUP = 8
ROWS = 32
CHUNK = 32
SMALL = 4


def split3(value):
    high = value.astype(jnp.bfloat16)
    rest = value - high.astype(jnp.float32)
    middle = rest.astype(jnp.bfloat16)
    low = (rest - middle.astype(jnp.float32)).astype(jnp.bfloat16)
    return jnp.concatenate([high, middle, low], axis=0)


def join3(value):
    rows = value.shape[0] // 3
    return value[:rows] + (value[rows : 2 * rows] + value[2 * rows :])


def kernel(
    sizes,
    pos, mass, cen, rad, blocks, halos,
    cen_out, rad_out, prof_out,
    raw_pos, raw_mass, raw_pair, data, pick, points, onehot, terms, state, asked,
    local_sem, send_sem, recv_sem, ready,
):
    ndx, ndy, slots, count = sizes
    n = ndx * ndy
    half = n // 2
    groups = n // GROUP
    halo_dev = rad.shape[1]
    mx = lax.axis_index("dx")
    my = lax.axis_index("dy")
    me = mx * ndy + my
    core = lax.rem(mx, 2)
    size_a, size_b, size_c = ndx // 2, 2, ndy // 2
    MESH = pl.DeviceIdType.MESH

    def flip(value, step, size):
        if size & (size - 1):
            return lax.rem(value + step, size)
        bit = 1
        while bit < size:
            if step & bit:
                value = value + bit * (1 - 2 * lax.rem(value // bit, 2))
            bit *= 2
        return value

    def at_step(step3, step2, step1):
        a, b, c = mx // 2, lax.rem(my, 2), my // 2
        c = flip(c, step1, size_c)
        if size_a == size_b:
            a0, b0 = flip(a, step3, size_a), flip(b, step2, size_b)
            a1, b1 = flip(a, step2, size_a), flip(b, step3, size_b)
            a, b = a0 + core * (a1 - a0), b0 + core * (b1 - b0)
        else:
            a, b = flip(a, step3, size_a), flip(b, step2, size_b)
        return 2 * a + core, 2 * c + b

    sibling = (mx + 1 - 2 * core, my)
    row_me = (me * slots) // 128
    pair_rows = raw_pair.shape[1]

    def label(p3, p2, p1):
        return (p3 * size_b + p2) * size_c + p1

    line = list(range(size_c))
    plane = [(p3, p2) for p3 in range(size_a) for p2 in range(size_b) if p3 or p2]
    plane.sort(key=lambda p: -(p[0] > 0) - (p[1] > 0))

    rank = []
    for p1 in line:
        rank.append((0, p1, 0, label(0, 0, p1)))
        rank.append((0, p1, 1, label(0, 0, p1) + half))
        for p3, p2 in plane:
            rank.append((1, p1, 0, label(p3, p2, p1)))
            rank.append((1, p1, 1, label(p3, p2, p1) + half))
    rank.sort()
    place_of = {t: i for i, (_, _, _, t) in enumerate(rank)}

    def lane_of(t):
        return t - 1 if t < half else half - 1 + place_of[t] // GROUP

    def copy(source, target, device):
        return pltpu.make_async_remote_copy(
            src_ref=data.at[place_of[source]], dst_ref=data.at[place_of[target]],
            send_sem=send_sem.at[0], recv_sem=recv_sem.at[lane_of(target)],
            device_id=device, device_id_type=MESH,
        )

    def several(size, lane):
        return pltpu.make_async_remote_copy(
            src_ref=data.at[pl.ds(0, size)], dst_ref=data.at[pl.ds(0, size)],
            send_sem=send_sem.at[0], recv_sem=recv_sem.at[lane],
            device_id=sibling, device_id_type=MESH,
        )

    zed = my // 2
    spot = (mx // 2) * size_b + lax.rem(my, 2)

    def outer_line(step):
        return flip(zed, step, size_c) > zed

    def outer_plane(p3, p2):
        tx, ty = at_step(p3, p2, 0)
        return (tx // 2) * size_b + lax.rem(ty, 2) > spot

    peers = [(0, 0, step) for step in line[1:]] + [(p3, p2, 0) for p3, p2 in plane]
    peers.sort(key=lambda p: (p[0] > 0) + (p[1] > 0) + p[2])

    cross = size_a == 2 and size_c <= SMALL
    tie = lax.rem(mx // 2 + lax.rem(my, 2), 2) == 1

    def outer(peer):
        if peer[2]:
            return outer_line(peer[2])
        return outer_plane(peer[0], peer[1])

    def diagonal(peer):
        return cross and peer[0] > 0 and peer[1] > 0

    def within(peer):
        inner = jnp.logical_not(outer(peer))
        return jnp.logical_and(inner, jnp.logical_not(tie)) if diagonal(peer) else inner

    def beyond(peer):
        return jnp.logical_or(outer(peer), tie) if diagonal(peer) else outer(peer)

    def greeted(peer):
        return jnp.logical_and(outer(peer), jnp.logical_not(tie)) if diagonal(peer) else outer(peer)

    def mark(peer):
        return ready.at[peer[2] if max(peer[:2]) == 0 else size_c + plane.index((peer[0], peer[1]))]

    def offer(peer):
        return copy(0, label(*peer), at_step(*peer))

    def spread(t):
        return [copy(t, label(p3, p2, t), at_step(p3, p2, 0)) for p3, p2 in plane]

    def hand_over(t):
        return copy(t, t + half, sibling)

    def relay(t):
        if 0 < t < size_c:
            for one in spread(t):
                one.start()
        if t < half:
            hand_over(t).start()

    def arrive(t):
        copy(0, t, sibling).wait_recv()
        relay(t)

    def answered(peer):
        pl.semaphore_wait(mark(peer), 1)
        offer(peer).start()

    def answer(peer, device):
        pl.semaphore_signal(mark(peer), inc=1, device_id=device, device_id_type=MESH)

    def begin():
        for k in line if size_c <= SMALL else []:

            @pl.when(zed == k)
            def _(k=k):
                for target in range(k):
                    offer((0, 0, k ^ target)).start()

        for peer in reversed(peers):
            if peer[2] == 0 or size_c > SMALL:
                pl.when(within(peer))(offer(peer).start)

        @pl.when(core == 0)
        def _():
            pl.semaphore_wait(ready.at[0], 1)

        relay(0)
        for peer in peers:
            if (peer[2] == 0 and not diagonal(peer)) or size_c > SMALL:
                pl.when(outer(peer))(functools.partial(answered, peer))
        if cross:

            @pl.when(spot == 0)
            def _():
                for peer in peers:
                    if peer[2] == 0 and not diagonal(peer):
                        answer((1, 1, 0), at_step(*peer))

        if size_c > SMALL:
            for t in line[1:]:
                arrive(t)
            return
        for k in line:

            @pl.when(zed == k)
            def _(k=k):
                near = sorted(line[1:], key=lambda t: (abs((k ^ t) - k), -(k ^ t)))
                away = [(0, 0, t) for t in near if k ^ t > k]
                for peer in away if k else away[:1]:
                    answered(peer)
                for peer in peers:
                    if diagonal(peer):
                        pl.when(beyond(peer))(functools.partial(answered, peer))
                for t in near:
                    if not k and t != near[0]:
                        answered((0, 0, t))
                    arrive(t)

    own = [
        pltpu.make_async_copy(pos, raw_pos, local_sem.at[0]),
        pltpu.make_async_copy(mass, raw_mass, local_sem.at[1]),
        pltpu.make_async_copy(blocks, raw_pair.at[0], local_sem.at[2]),
        pltpu.make_async_copy(halos, raw_pair.at[1], local_sem.at[3]),
        pltpu.make_async_copy(cen, cen_out, local_sem.at[4]),
        pltpu.make_async_copy(rad, rad_out, local_sem.at[5]),
    ]
    barrier = pltpu.get_barrier_semaphore()

    def greet(device):
        pl.semaphore_signal(barrier, inc=1, device_id=device, device_id_type=MESH)

    for one in own:
        one.start()
    for peer in peers:
        pl.when(greeted(peer))(functools.partial(greet, at_step(*peer)))
    pl.when(core == 0)(functools.partial(greet, sibling))
    lower = zed + spot + core
    if cross:
        lower = lower - jnp.where(spot == 2, 1, 0)

    @pl.when(lower > 0)
    def _():
        pl.semaphore_wait(barrier, lower)

    for peer in peers:
        pl.when(within(peer))(functools.partial(answer, peer, at_step(*peer)))
    pl.when(core == 1)(functools.partial(answer, (0, 0, 0), sibling))
    for one in own:
        one.wait()
    mine = place_of[0]
    for b in range(count):
        part = raw_pos[:, b * BLOCK : (b + 1) * BLOCK]
        for i in range(3):
            data[mine, i * count + b : i * count + b + 1, :] = part[i : i + 1]
    data[mine, 3 * count : 4 * count, :] = raw_mass[...]
    for i in range(2):
        at = 4 * count + i * pair_rows
        data[mine, at : at + pair_rows, :] = raw_pair[i].astype(jnp.float32)
    state[...] = jnp.zeros_like(state)
    terms[...] = jnp.zeros_like(terms)
    state[0:3, :] = cen_out[...]
    state[3:4, :] = rad_out[...]
    begin()

    lane0 = me * slots - row_me * 128
    lanes = lax.broadcasted_iota(jnp.int32, (GROUP, halo_dev), 1).astype(jnp.float32)
    spots = lax.broadcasted_iota(jnp.int32, (GROUP, GROUP * count), 1).astype(jnp.float32)
    place = lax.broadcasted_iota(jnp.int32, (GROUP, 128), 0).astype(jnp.float32)
    shift = lax.rem(128 - lane0, 128)

    def prepare(g):
        lo = g * GROUP * slots
        if not isinstance(g, int):
            lo = pl.multiple_of(lo, GROUP * slots)

        def taken(i):
            at = 4 * count + i * pair_rows + row_me
            part = data[pl.ds(g * GROUP, GROUP), pl.ds(at, 1), :].reshape(GROUP, 128)
            return pltpu.roll(part, shift, 1)

        rows = taken(1)
        want = taken(0) + place * float(count)
        for j in range(0, slots, 2):
            start = lo + j * GROUP
            for values, iota, out in ((rows, lanes, onehot), (want, spots, pick)):
                pair = [
                    jnp.where(values[:, i : i + 1] == iota, 1.0, 0.0) for i in (j, j + 1)
                ]
                both = jnp.concatenate(pair, axis=0).astype(jnp.bfloat16)
                out[pl.ds(start, 2 * GROUP), :] = both
        asked[:, pl.ds(lo, GROUP * slots)] = join3(
            lax.dot_general(
                split3(state[...]), onehot[pl.ds(lo, GROUP * slots), :], (((1,), (1,)), ((), ())),
                preferred_element_type=jnp.float32,
            )
        )

    def ask():
        asked[...] = join3(
            lax.dot_general(
                split3(state[...]), onehot[...], (((1,), (1,)), ((), ())),
                preferred_element_type=jnp.float32,
            )
        )

    width = GROUP * slots

    def evaluate(g):
        lo = pl.multiple_of(g * width, width)
        mine = asked[0:4, pl.ds(lo, width)]
        cx, cy, cz, radius = (mine[i : i + 1] for i in range(4))
        scale = (SHELLS / 2.0) / jnp.where(radius > 0.0, radius, 1.0)

        def fold(value):
            return jnp.sum(value.reshape(CHUNK // 8, 8, width), axis=0)

        def chunk(c, acc):
            at = pl.ds(pl.multiple_of(c * CHUNK, CHUNK), CHUNK)
            ox = points[g, 0, at] - cx
            oy = points[g, 1, at] - cy
            oz = points[g, 2, at] - cz
            m = points[g, 3, at]
            u = jnp.sqrt(ox * ox + oy * oy + oz * oz) * scale
            ramp = m * (0.5 - u)
            out = []
            for k in range(SHELLS + 1):
                out.append(acc[k] + fold(jnp.maximum(ramp, 0.0)))
                ramp = ramp + m
            inner = m * jnp.clip(SHELLS / 2.0 - u, 0.0, 1.0)
            out.append(acc[SHELLS + 1] + fold(inner))
            for i, o in enumerate((ox, oy, oz)):
                out.append(acc[SHELLS + 2 + i] + fold(o * inner))
            return tuple(out)

        zero = jnp.zeros((8, width), jnp.float32)
        acc = lax.fori_loop(0, BLOCK // CHUNK, chunk, (zero,) * (SHELLS + 5))
        acc = [acc[k + 1] - acc[k] - acc[0] for k in range(SHELLS)] + list(acc[SHELLS + 1 :])
        for k in range(SHELLS + 4):
            terms[k : k + 1, pl.ds(lo, width)] = jnp.sum(acc[k], axis=0, keepdims=True)

    def choose(g):
        chosen = pick[pl.ds(pl.multiple_of(g * width, width), width), :]
        for i in range(4):
            flat = data[pl.ds(g * GROUP, GROUP), i * count : (i + 1) * count, :]
            flat = flat.reshape(GROUP * count, BLOCK).T
            points[g, i] = join3(
                lax.dot_general(
                    split3(flat), chosen, (((1,), (1,)), ((), ())),
                    preferred_element_type=jnp.float32,
                )
            )

    def compute(g):
        choose(g)
        evaluate(g)

    def again(g, _):
        evaluate(g)
        return 0

    def advance():
        sums = join3(
            lax.dot_general(
                split3(terms[...]), onehot[...], (((1,), (0,)), ((), ())),
                preferred_element_type=jnp.float32,
            )
        )
        radius = state[3:4, :]
        enclosed = sums[SHELLS // 2 - 1 : SHELLS // 2]
        ratio = (1.0 + enclosed) / (1.0 + radius * radius * radius)
        state[3:4, :] = radius * jnp.exp(jnp.log(ratio) * (1.0 / 3.0))
        total = jnp.maximum(sums[SHELLS : SHELLS + 1], 1.0)
        state[0:3, :] = state[0:3, :] + sums[SHELLS + 1 : SHELLS + 4] / total
        return sums

    level = [rank[i][1] if rank[i][0] else -1 for i in range(n)]
    done = 0
    for p1 in line:
        for p3, p2 in reversed(plane):
            arrive(label(p3, p2, p1))
        while done < groups and (p1 == line[-1] or level[(done + 1) * GROUP - 1] < p1):
            late = sum(rank[i][3] >= half for i in range(done * GROUP, (done + 1) * GROUP))
            if late:
                several(late, half - 1 + done).wait_recv()
            prepare(done)
            compute(done)
            done += 1
    sums = advance()
    for step in range(1, ITERS):
        ask()
        lax.fori_loop(0, groups, again, 0)
        sums = advance()
    cen_out[...] = state[0:3, :]
    rad_out[...] = state[3:4, :]
    prof_out[...] = sums[:SHELLS]
    several(n - 1, 0).wait_send()


def hand(a, b, c, x, y, z, sem):
    copies = [
        pltpu.make_async_copy(source, target, sem.at[i])
        for i, (source, target) in enumerate(((a, x), (b, y), (c, z)))
    ]
    for copy in copies:
        copy.start()
    for copy in copies:
        copy.wait()


def body(positions, masses, centers, radii, pair_block, pair_halo):
    ndx = lax.axis_size("dx")
    ndy = lax.axis_size("dy")
    n = ndx * ndy
    halo_dev = radii.shape[0]
    count = masses.shape[0] // BLOCK
    slots = pair_halo.shape[0] // n
    total = n * slots
    groups = n // GROUP
    any_ref = pl.BlockSpec(memory_space=pl.ANY)
    vmem = pl.BlockSpec(memory_space=pltpu.VMEM)
    f32 = jnp.float32
    dma = pltpu.SemaphoreType.DMA
    out = pl.pallas_call(
        functools.partial(kernel, (ndx, ndy, slots, count)),
        out_shape=(
            pltpu.VMEM((3, halo_dev), f32),
            pltpu.VMEM((1, halo_dev), f32),
            pltpu.VMEM((SHELLS, halo_dev), f32),
        ),
        in_specs=[any_ref] * 6,
        out_specs=(vmem,) * 3,
        scratch_shapes=[
            pltpu.VMEM((3, count * BLOCK), f32),
            pltpu.VMEM((count, BLOCK), f32),
            pltpu.VMEM((2, total // 128, 128), jnp.int32),
            pltpu.VMEM((n, 4 * count + 2 * (total // 128), BLOCK), f32),
            pltpu.VMEM((total, GROUP * count), jnp.bfloat16),
            pltpu.VMEM((groups, 4, BLOCK, GROUP * slots), f32),
            pltpu.VMEM((total, halo_dev), jnp.bfloat16),
            pltpu.VMEM((ROWS, total), f32),
            pltpu.VMEM((16, halo_dev), f32),
            pltpu.VMEM((16, total), f32),
            dma((6,)),
            dma((1,)),
            dma((n // 2 - 1 + groups,)),
            pltpu.SemaphoreType.REGULAR((ndx + ndy // 2,)),
        ],
        compiler_params=pltpu.CompilerParams(collective_id=0, has_side_effects=True),
    )(
        positions,
        masses.reshape(count, BLOCK),
        centers,
        radii.reshape(1, halo_dev),
        pair_block.reshape(total // 128, 128),
        pair_halo.reshape(total // 128, 128),
    )
    out = [pltpu.with_memory_space_constraint(x, pltpu.VMEM) for x in out]
    out = pl.pallas_call(
        hand,
        out_shape=tuple(jax.ShapeDtypeStruct(x.shape, f32) for x in out),
        in_specs=[vmem] * 3,
        out_specs=(any_ref,) * 3,
        scratch_shapes=[dma((3,))],
    )(*out)
    return out[0], out[1].reshape(halo_dev), out[2]


def solution(mesh):
    flat = P(("dx", "dy"))
    rows = P(None, ("dx", "dy"))
    in_specs = (rows, flat, rows, flat, flat, flat)
    out_specs = (rows, flat, rows)
    return jax.shard_map(body, mesh=mesh, in_specs=in_specs, out_specs=out_specs, check_vma=False)
```

```python
import functools

import jax
import jax.numpy as jnp
from jax import lax
from jax.experimental import pallas as pl
from jax.experimental.pallas import tpu as pltpu
from jax.sharding import PartitionSpec as P

SHELLS = 16
BLOCK = 128
ITERS = 2
GROUP = 8
ROWS = 32
CHUNK = 32
SMALL = 4


def split3(value):
    high = value.astype(jnp.bfloat16)
    rest = value - high.astype(jnp.float32)
    middle = rest.astype(jnp.bfloat16)
    low = (rest - middle.astype(jnp.float32)).astype(jnp.bfloat16)
    return jnp.concatenate([high, middle, low], axis=0)


def join3(value):
    rows = value.shape[0] // 3
    return value[:rows] + (value[rows : 2 * rows] + value[2 * rows :])


def kernel(
    sizes,
    pos, mass, cen, rad, blocks, halos,
    cen_out, rad_out, prof_out,
    raw_pos, raw_mass, raw_pair, asking, data, pick, points, onehot, terms, state, asked,
    local_sem, send_sem, recv_sem, ready,
):
    ndx, ndy, slots, count = sizes
    n = ndx * ndy
    half = n // 2
    groups = n // GROUP
    halo_dev = rad.shape[1]
    mx = lax.axis_index("dx")
    my = lax.axis_index("dy")
    me = mx * ndy + my
    core = lax.rem(mx, 2)
    size_a, size_b, size_c = ndx // 2, 2, ndy // 2
    MESH = pl.DeviceIdType.MESH

    def flip(value, step, size):
        if size & (size - 1):
            return lax.rem(value + step, size)
        bit = 1
        while bit < size:
            if step & bit:
                value = value + bit * (1 - 2 * lax.rem(value // bit, 2))
            bit *= 2
        return value

    def at_step(step3, step2, step1):
        a, b, c = mx // 2, lax.rem(my, 2), my // 2
        c = flip(c, step1, size_c)
        if size_a == size_b:
            a0, b0 = flip(a, step3, size_a), flip(b, step2, size_b)
            a1, b1 = flip(a, step2, size_a), flip(b, step3, size_b)
            a, b = a0 + core * (a1 - a0), b0 + core * (b1 - b0)
        else:
            a, b = flip(a, step3, size_a), flip(b, step2, size_b)
        return 2 * a + core, 2 * c + b

    sibling = (mx + 1 - 2 * core, my)
    share = size_b * slots
    asks = ndx * share // 128
    body_rows = 4 * count
    row_me = mx * share // 128

    def label(p3, p2, p1):
        return (p3 * size_b + p2) * size_c + p1

    line = list(range(size_c))
    plane = [(p3, p2) for p3 in range(size_a) for p2 in range(size_b) if p3 or p2]
    plane.sort(key=lambda p: -(p[0] > 0) - (p[1] > 0))

    rank = []
    for p1 in line:
        rank.append((0, p1, 0, label(0, 0, p1)))
        rank.append((0, p1, 1, label(0, 0, p1) + half))
        for p3, p2 in plane:
            rank.append((1, p1, 0, label(p3, p2, p1)))
            rank.append((1, p1, 1, label(p3, p2, p1) + half))
    rank.sort()
    place_of = {t: i for i, (_, _, _, t) in enumerate(rank)}

    def lane_of(t):
        return t - 1 if t < half else half - 1 + place_of[t] // GROUP

    def copy(source, target, device):
        rows = body_rows if source == 0 and target < size_c else body_rows + 2 * asks
        if source == target:
            rows = body_rows + 2 * asks
        return pltpu.make_async_remote_copy(
            src_ref=data.at[place_of[source], pl.ds(0, rows)],
            dst_ref=data.at[place_of[target], pl.ds(0, rows)],
            send_sem=send_sem.at[0], recv_sem=recv_sem.at[lane_of(target)],
            device_id=device, device_id_type=MESH,
        )

    def wanted(step, device):
        slot = place_of[step]
        return pltpu.make_async_remote_copy(
            src_ref=asking.at[at_step(0, 0, step)[1] // 2],
            dst_ref=data.at[slot, pl.ds(body_rows, 2 * asks)],
            send_sem=send_sem.at[0], recv_sem=recv_sem.at[lane_of(step)],
            device_id=device, device_id_type=MESH,
        )

    def several(size, lane):
        return pltpu.make_async_remote_copy(
            src_ref=data.at[pl.ds(0, size)], dst_ref=data.at[pl.ds(0, size)],
            send_sem=send_sem.at[0], recv_sem=recv_sem.at[lane],
            device_id=sibling, device_id_type=MESH,
        )

    zed = my // 2
    spot = (mx // 2) * size_b + lax.rem(my, 2)

    def outer_line(step):
        return flip(zed, step, size_c) > zed

    def outer_plane(p3, p2):
        tx, ty = at_step(p3, p2, 0)
        return (tx // 2) * size_b + lax.rem(ty, 2) > spot

    peers = [(0, 0, step) for step in line[1:]] + [(p3, p2, 0) for p3, p2 in plane]
    peers.sort(key=lambda p: (p[0] > 0) + (p[1] > 0) + p[2])

    cross = size_a == 2 and size_c <= SMALL
    tie = lax.rem(mx // 2 + lax.rem(my, 2), 2) == 1

    def outer(peer):
        if peer[2]:
            return outer_line(peer[2])
        return outer_plane(peer[0], peer[1])

    def diagonal(peer):
        return cross and peer[0] > 0 and peer[1] > 0

    def within(peer):
        inner = jnp.logical_not(outer(peer))
        return jnp.logical_and(inner, jnp.logical_not(tie)) if diagonal(peer) else inner

    def beyond(peer):
        return jnp.logical_or(outer(peer), tie) if diagonal(peer) else outer(peer)

    def greeted(peer):
        return jnp.logical_and(outer(peer), jnp.logical_not(tie)) if diagonal(peer) else outer(peer)

    def mark(peer):
        return ready.at[peer[2] if max(peer[:2]) == 0 else size_c + plane.index((peer[0], peer[1]))]

    class Pair:
        def __init__(self, *parts):
            self.parts = parts

        def start(self):
            for part in self.parts:
                part.start()

    def offer(peer):
        one = copy(0, label(*peer), at_step(*peer))
        if peer[2]:
            return Pair(one, wanted(peer[2], at_step(*peer)))
        return one

    def spread(t):
        return [copy(t, label(p3, p2, t), at_step(p3, p2, 0)) for p3, p2 in plane]

    def hand_over(t):
        return copy(t, t + half, sibling)

    def relay(t):
        if 0 < t < size_c:
            if cross:
                corner, *sides = spread(t)
                pl.when(spot == 3)(corner.start)
                for one in sides:
                    one.start()
                pl.when(spot != 3)(corner.start)
            else:
                for one in spread(t):
                    one.start()
        if t < half:
            hand_over(t).start()

    def arrive(t):
        copy(t, t, sibling).wait_recv()
        relay(t)

    def answered(peer):
        pl.semaphore_wait(mark(peer), 1)
        offer(peer).start()

    def answer(peer, device):
        pl.semaphore_signal(mark(peer), inc=1, device_id=device, device_id_type=MESH)

    def begin():
        for k in line if size_c <= SMALL else []:

            @pl.when(zed == k)
            def _(k=k):
                for target in range(k):
                    offer((0, 0, k ^ target)).start()

        for peer in reversed(peers):
            if peer[2] == 0 or size_c > SMALL:
                pl.when(within(peer))(offer(peer).start)

        @pl.when(core == 0)
        def _():
            pl.semaphore_wait(ready.at[0], 1)

        relay(0)
        for peer in peers:
            if (peer[2] == 0 and not diagonal(peer)) or size_c > SMALL:
                pl.when(outer(peer))(functools.partial(answered, peer))
        if cross:

            @pl.when(spot == 0)
            def _():
                for peer in peers:
                    if peer[2] == 0 and not diagonal(peer):
                        answer((1, 1, 0), at_step(*peer))

        if size_c > SMALL:
            for t in line[1:]:
                arrive(t)
            return
        for k in line:

            @pl.when(zed == k)
            def _(k=k):
                near = sorted(line[1:], key=lambda t: (abs((k ^ t) - k), k ^ t))
                away = [(0, 0, t) for t in near if k ^ t > k]
                for peer in away:
                    answered(peer)
                for peer in peers:
                    if diagonal(peer):
                        pl.when(beyond(peer))(functools.partial(answered, peer))
                for t in near:
                    arrive(t)

    own = [
        pltpu.make_async_copy(pos, raw_pos, local_sem.at[0]),
        pltpu.make_async_copy(mass, raw_mass, local_sem.at[1]),
        pltpu.make_async_copy(blocks, raw_pair.at[0], local_sem.at[2]),
        pltpu.make_async_copy(halos, raw_pair.at[1], local_sem.at[3]),
        pltpu.make_async_copy(cen, cen_out, local_sem.at[4]),
        pltpu.make_async_copy(rad, rad_out, local_sem.at[5]),
    ]
    barrier = pltpu.get_barrier_semaphore()

    def greet(device):
        pl.semaphore_signal(barrier, inc=1, device_id=device, device_id_type=MESH)

    for one in own:
        one.start()
    for peer in peers:
        pl.when(greeted(peer))(functools.partial(greet, at_step(*peer)))
    pl.when(core == 0)(functools.partial(greet, sibling))
    lower = zed + spot + core
    if cross:
        lower = lower - jnp.where(spot == 2, 1, 0)

    @pl.when(lower > 0)
    def _():
        pl.semaphore_wait(barrier, lower)

    for peer in peers:
        pl.when(within(peer))(functools.partial(answer, peer, at_step(*peer)))
    pl.when(core == 1)(functools.partial(answer, (0, 0, 0), sibling))
    for one in own:
        one.wait()
    mine = place_of[0]
    for b in range(count):
        part = raw_pos[:, b * BLOCK : (b + 1) * BLOCK]
        for i in range(3):
            data[mine, i * count + b : i * count + b + 1, :] = part[i : i + 1]
    data[mine, 3 * count : 4 * count, :] = raw_mass[...]
    groups_of = lax.broadcasted_iota(jnp.int32, (1, 128), 1) // share
    for i in range(2):
        values = raw_pair[i].astype(jnp.float32)
        turned = {0: values}
        for z in line:
            for row in range(asks):
                total = jnp.zeros((1, 128), jnp.float32)
                for part in range(128 // share):
                    start = ((row * (128 // share) + part) * size_c + z) * share
                    turn = (part * share - start) % 128
                    if turn not in turned:
                        turned[turn] = pltpu.roll(values, turn, 1)
                    piece = turned[turn][start // 128 : start // 128 + 1]
                    total = jnp.where(groups_of == part, piece, total)
                asking[z, i * asks + row : i * asks + row + 1, :] = total
    data[mine, pl.ds(body_rows, 2 * asks), :] = asking[zed]
    state[...] = jnp.zeros_like(state)
    terms[...] = jnp.zeros_like(terms)
    state[0:3, :] = cen_out[...]
    state[3:4, :] = rad_out[...]
    begin()

    lane0 = lax.rem(mx * share, 128) + lax.rem(my, 2) * slots
    lanes = lax.broadcasted_iota(jnp.int32, (GROUP, halo_dev), 1).astype(jnp.float32)
    spots = lax.broadcasted_iota(jnp.int32, (GROUP, GROUP * count), 1).astype(jnp.float32)
    place = lax.broadcasted_iota(jnp.int32, (GROUP, 128), 0).astype(jnp.float32)
    shift = lax.rem(128 - lane0, 128)

    def prepare(g):
        lo = g * GROUP * slots
        if not isinstance(g, int):
            lo = pl.multiple_of(lo, GROUP * slots)

        def taken(i):
            at = body_rows + i * asks + row_me
            part = data[pl.ds(g * GROUP, GROUP), pl.ds(at, 1), :].reshape(GROUP, 128)
            return pltpu.roll(part, shift, 1)

        rows = taken(1)
        want = taken(0) + place * float(count)
        for j in range(0, slots, 2):
            start = lo + j * GROUP
            for values, iota, out in ((rows, lanes, onehot), (want, spots, pick)):
                pair = [
                    jnp.where(values[:, i : i + 1] == iota, 1.0, 0.0) for i in (j, j + 1)
                ]
                both = jnp.concatenate(pair, axis=0).astype(jnp.bfloat16)
                out[pl.ds(start, 2 * GROUP), :] = both
        asked[:, pl.ds(lo, GROUP * slots)] = join3(
            lax.dot_general(
                split3(state[...]), onehot[pl.ds(lo, GROUP * slots), :], (((1,), (1,)), ((), ())),
                preferred_element_type=jnp.float32,
            )
        )

    def ask():
        asked[...] = join3(
            lax.dot_general(
                split3(state[...]), onehot[...], (((1,), (1,)), ((), ())),
                preferred_element_type=jnp.float32,
            )
        )

    width = GROUP * slots

    def evaluate(g):
        lo = pl.multiple_of(g * width, width)
        mine = asked[0:4, pl.ds(lo, width)]
        cx, cy, cz, radius = (mine[i : i + 1] for i in range(4))
        scale = (SHELLS / 2.0) / jnp.where(radius > 0.0, radius, 1.0)

        def fold(value):
            return jnp.sum(value.reshape(CHUNK // 8, 8, width), axis=0)

        def chunk(c, acc):
            at = pl.ds(pl.multiple_of(c * CHUNK, CHUNK), CHUNK)
            ox = points[g, 0, at] - cx
            oy = points[g, 1, at] - cy
            oz = points[g, 2, at] - cz
            m = points[g, 3, at]
            u = jnp.sqrt(ox * ox + oy * oy + oz * oz) * scale
            ramp = m * (0.5 - u)
            out = []
            for k in range(SHELLS + 1):
                out.append(acc[k] + fold(jnp.maximum(ramp, 0.0)))
                ramp = ramp + m
            inner = m * jnp.clip(SHELLS / 2.0 - u, 0.0, 1.0)
            out.append(acc[SHELLS + 1] + fold(inner))
            for i, o in enumerate((ox, oy, oz)):
                out.append(acc[SHELLS + 2 + i] + fold(o * inner))
            return tuple(out)

        zero = jnp.zeros((8, width), jnp.float32)
        acc = lax.fori_loop(0, BLOCK // CHUNK, chunk, (zero,) * (SHELLS + 5))
        acc = [acc[k + 1] - acc[k] - acc[0] for k in range(SHELLS)] + list(acc[SHELLS + 1 :])
        for k in range(SHELLS + 4):
            terms[k : k + 1, pl.ds(lo, width)] = jnp.sum(acc[k], axis=0, keepdims=True)

    def choose(g):
        chosen = pick[pl.ds(pl.multiple_of(g * width, width), width), :]
        for i in range(4):
            flat = data[pl.ds(g * GROUP, GROUP), i * count : (i + 1) * count, :]
            flat = flat.reshape(GROUP * count, BLOCK).T
            points[g, i] = join3(
                lax.dot_general(
                    split3(flat), chosen, (((1,), (1,)), ((), ())),
                    preferred_element_type=jnp.float32,
                )
            )

    def compute(g):
        choose(g)
        evaluate(g)

    def again(g, _):
        evaluate(g)
        return 0

    def advance():
        sums = join3(
            lax.dot_general(
                split3(terms[...]), onehot[...], (((1,), (0,)), ((), ())),
                preferred_element_type=jnp.float32,
            )
        )
        radius = state[3:4, :]
        enclosed = sums[SHELLS // 2 - 1 : SHELLS // 2]
        ratio = (1.0 + enclosed) / (1.0 + radius * radius * radius)
        state[3:4, :] = radius * jnp.exp(jnp.log(ratio) * (1.0 / 3.0))
        total = jnp.maximum(sums[SHELLS : SHELLS + 1], 1.0)
        state[0:3, :] = state[0:3, :] + sums[SHELLS + 1 : SHELLS + 4] / total
        return sums

    def plane_of(p1):
        for p3, p2 in reversed(plane):
            arrive(label(p3, p2, p1))

    def finish(g):
        late = sum(rank[i][3] >= half for i in range(g * GROUP, (g + 1) * GROUP))
        if late:
            several(late, half - 1 + g).wait_recv()
        prepare(g)
        compute(g)

    def closer(k):
        return sorted(line[1:], key=lambda t: (abs((k ^ t) - k), k ^ t))

    plane_of(0)
    finish(0)
    if size_c <= SMALL:
        for k in line:

            @pl.when(zed == k)
            def _(k=k):
                for i, p1 in enumerate(closer(k)):
                    plane_of(p1)
                    if k == 0 and i == 0:
                        finish(1)

        pl.when(zed > 0)(functools.partial(finish, 1))
    else:
        for p1 in line[1:]:
            plane_of(p1)
        finish(1)
    for g in range(2, groups):
        finish(g)
    sums = advance()
    for step in range(1, ITERS):
        ask()
        lax.fori_loop(0, groups, again, 0)
        sums = advance()
    cen_out[...] = state[0:3, :]
    rad_out[...] = state[3:4, :]
    prof_out[...] = sums[:SHELLS]
    several(n - 1, 0).wait_send()


def hand(a, b, c, x, y, z, sem):
    copies = [
        pltpu.make_async_copy(source, target, sem.at[i])
        for i, (source, target) in enumerate(((a, x), (b, y), (c, z)))
    ]
    for copy in copies:
        copy.start()
    for copy in copies:
        copy.wait()


def body(positions, masses, centers, radii, pair_block, pair_halo):
    ndx = lax.axis_size("dx")
    ndy = lax.axis_size("dy")
    n = ndx * ndy
    halo_dev = radii.shape[0]
    count = masses.shape[0] // BLOCK
    slots = pair_halo.shape[0] // n
    total = n * slots
    groups = n // GROUP
    any_ref = pl.BlockSpec(memory_space=pl.ANY)
    vmem = pl.BlockSpec(memory_space=pltpu.VMEM)
    f32 = jnp.float32
    dma = pltpu.SemaphoreType.DMA
    out = pl.pallas_call(
        functools.partial(kernel, (ndx, ndy, slots, count)),
        out_shape=(
            pltpu.VMEM((3, halo_dev), f32),
            pltpu.VMEM((1, halo_dev), f32),
            pltpu.VMEM((SHELLS, halo_dev), f32),
        ),
        in_specs=[any_ref] * 6,
        out_specs=(vmem,) * 3,
        scratch_shapes=[
            pltpu.VMEM((3, count * BLOCK), f32),
            pltpu.VMEM((count, BLOCK), f32),
            pltpu.VMEM((2, total // 128, 128), jnp.int32),
            pltpu.VMEM((ndy // 2, ndx * slots // 32, BLOCK), f32),
            pltpu.VMEM((n, 4 * count + ndx * slots // 32, BLOCK), f32),
            pltpu.VMEM((total, GROUP * count), jnp.bfloat16),
            pltpu.VMEM((groups, 4, BLOCK, GROUP * slots), f32),
            pltpu.VMEM((total, halo_dev), jnp.bfloat16),
            pltpu.VMEM((ROWS, total), f32),
            pltpu.VMEM((16, halo_dev), f32),
            pltpu.VMEM((16, total), f32),
            dma((6,)),
            dma((1,)),
            dma((n // 2 - 1 + groups,)),
            pltpu.SemaphoreType.REGULAR((ndx + ndy // 2,)),
        ],
        compiler_params=pltpu.CompilerParams(collective_id=0, has_side_effects=True),
    )(
        positions,
        masses.reshape(count, BLOCK),
        centers,
        radii.reshape(1, halo_dev),
        pair_block.reshape(total // 128, 128),
        pair_halo.reshape(total // 128, 128),
    )
    out = [pltpu.with_memory_space_constraint(x, pltpu.VMEM) for x in out]
    out = pl.pallas_call(
        hand,
        out_shape=tuple(jax.ShapeDtypeStruct(x.shape, f32) for x in out),
        in_specs=[vmem] * 3,
        out_specs=(any_ref,) * 3,
        scratch_shapes=[dma((3,))],
    )(*out)
    return out[0], out[1].reshape(halo_dev), out[2]


def solution(mesh):
    flat = P(("dx", "dy"))
    rows = P(None, ("dx", "dy"))
    in_specs = (rows, flat, rows, flat, flat, flat)
    out_specs = (rows, flat, rows)
    return jax.shard_map(body, mesh=mesh, in_specs=in_specs, out_specs=out_specs, check_vma=False)
```

```python
import functools

import jax
import jax.numpy as jnp
from jax import lax
from jax.experimental import pallas as pl
from jax.experimental.pallas import tpu as pltpu
from jax.sharding import PartitionSpec as P

SHELLS = 16
BLOCK = 128
KEEP = 24
GROUP = 8
ROWS = 32
CHUNK = 32
SMALL = 4


def split3(value):
    high = value.astype(jnp.bfloat16)
    rest = value - high.astype(jnp.float32)
    middle = rest.astype(jnp.bfloat16)
    low = (rest - middle.astype(jnp.float32)).astype(jnp.bfloat16)
    return jnp.concatenate([high, middle, low], axis=0)


def join3(value):
    rows = value.shape[0] // 3
    return value[:rows] + (value[rows : 2 * rows] + value[2 * rows :])


def kernel(
    sizes,
    pos, mass, cen, rad, blocks, halos,
    cen_out, rad_out, prof_out,
    raw_pos, raw_mass, raw_pair, asking, data, pick, points, onehot, cols, same, terms, state, asked,
    local_sem, send_sem, recv_sem, ready,
):
    ndx, ndy, slots, count = sizes
    n = ndx * ndy
    half = n // 2
    groups = n // GROUP
    halo_dev = rad.shape[1]
    mx = lax.axis_index("dx")
    my = lax.axis_index("dy")
    me = mx * ndy + my
    core = lax.rem(mx, 2)
    size_a, size_b, size_c = ndx // 2, 2, ndy // 2
    MESH = pl.DeviceIdType.MESH

    def flip(value, step, size):
        if size & (size - 1):
            return lax.rem(value + step, size)
        bit = 1
        while bit < size:
            if step & bit:
                value = value + bit * (1 - 2 * lax.rem(value // bit, 2))
            bit *= 2
        return value

    def at_step(step3, step2, step1):
        a, b, c = mx // 2, lax.rem(my, 2), my // 2
        c = flip(c, step1, size_c)
        if size_a == size_b:
            a0, b0 = flip(a, step3, size_a), flip(b, step2, size_b)
            a1, b1 = flip(a, step2, size_a), flip(b, step3, size_b)
            a, b = a0 + core * (a1 - a0), b0 + core * (b1 - b0)
        else:
            a, b = flip(a, step3, size_a), flip(b, step2, size_b)
        return 2 * a + core, 2 * c + b

    sibling = (mx + 1 - 2 * core, my)
    share = size_b * slots
    asks = ndx * share // 128
    body_rows = 4 * count
    row_me = mx * share // 128

    def label(p3, p2, p1):
        return (p3 * size_b + p2) * size_c + p1

    line = list(range(size_c))
    plane = [(p3, p2) for p3 in range(size_a) for p2 in range(size_b) if p3 or p2]
    plane.sort(key=lambda p: -(p[0] > 0) - (p[1] > 0))

    rank = []
    for p1 in line:
        rank.append((0, p1, 0, label(0, 0, p1)))
        rank.append((0, p1, 1, label(0, 0, p1) + half))
        for p3, p2 in plane:
            rank.append((1, p1, 0, label(p3, p2, p1)))
            rank.append((1, p1, 1, label(p3, p2, p1) + half))
    rank.sort()
    place_of = {t: i for i, (_, _, _, t) in enumerate(rank)}

    def lane_of(t):
        return t - 1 if t < half else half - 1 + place_of[t] // GROUP

    def copy(source, target, device):
        rows = body_rows if source == 0 and target < size_c else body_rows + 2 * asks
        if source == target:
            rows = body_rows + 2 * asks
        return pltpu.make_async_remote_copy(
            src_ref=data.at[place_of[source], pl.ds(0, rows)],
            dst_ref=data.at[place_of[target], pl.ds(0, rows)],
            send_sem=send_sem.at[0], recv_sem=recv_sem.at[lane_of(target)],
            device_id=device, device_id_type=MESH,
        )

    def wanted(step, device):
        slot = place_of[step]
        return pltpu.make_async_remote_copy(
            src_ref=asking.at[at_step(0, 0, step)[1] // 2],
            dst_ref=data.at[slot, pl.ds(body_rows, 2 * asks)],
            send_sem=send_sem.at[0], recv_sem=recv_sem.at[lane_of(step)],
            device_id=device, device_id_type=MESH,
        )

    def several(size, lane):
        return pltpu.make_async_remote_copy(
            src_ref=data.at[pl.ds(0, size)], dst_ref=data.at[pl.ds(0, size)],
            send_sem=send_sem.at[0], recv_sem=recv_sem.at[lane],
            device_id=sibling, device_id_type=MESH,
        )

    zed = my // 2
    spot = (mx // 2) * size_b + lax.rem(my, 2)

    def outer_line(step):
        return flip(zed, step, size_c) > zed

    def outer_plane(p3, p2):
        tx, ty = at_step(p3, p2, 0)
        return (tx // 2) * size_b + lax.rem(ty, 2) > spot

    peers = [(0, 0, step) for step in line[1:]] + [(p3, p2, 0) for p3, p2 in plane]
    peers.sort(key=lambda p: (p[0] > 0) + (p[1] > 0) + p[2])

    cross = size_a == 2 and size_c <= SMALL
    tie = lax.rem(mx // 2 + lax.rem(my, 2), 2) == 1

    def outer(peer):
        if peer[2]:
            return outer_line(peer[2])
        return outer_plane(peer[0], peer[1])

    def diagonal(peer):
        return cross and peer[0] > 0 and peer[1] > 0

    def within(peer):
        inner = jnp.logical_not(outer(peer))
        return jnp.logical_and(inner, jnp.logical_not(tie)) if diagonal(peer) else inner

    def beyond(peer):
        return jnp.logical_or(outer(peer), tie) if diagonal(peer) else outer(peer)

    def greeted(peer):
        return jnp.logical_and(outer(peer), jnp.logical_not(tie)) if diagonal(peer) else outer(peer)

    def mark(peer):
        return ready.at[peer[2] if max(peer[:2]) == 0 else size_c + plane.index((peer[0], peer[1]))]

    class Pair:
        def __init__(self, *parts):
            self.parts = parts

        def start(self):
            for part in self.parts:
                part.start()

    def offer(peer):
        one = copy(0, label(*peer), at_step(*peer))
        if peer[2]:
            return Pair(one, wanted(peer[2], at_step(*peer)))
        return one

    def spread(t):
        return [copy(t, label(p3, p2, t), at_step(p3, p2, 0)) for p3, p2 in plane]

    def hand_over(t):
        return copy(t, t + half, sibling)

    def relay(t):
        if 0 < t < size_c:
            if cross:
                corner, *sides = spread(t)
                pl.when(spot == 3)(corner.start)
                for one in sides:
                    one.start()
                pl.when(spot != 3)(corner.start)
            else:
                for one in spread(t):
                    one.start()
        if t < half:
            hand_over(t).start()

    def arrive(t):
        copy(t, t, sibling).wait_recv()
        relay(t)

    def answered(peer):
        pl.semaphore_wait(mark(peer), 1)
        offer(peer).start()

    def answer(peer, device):
        pl.semaphore_signal(mark(peer), inc=1, device_id=device, device_id_type=MESH)

    def begin():
        for k in line if size_c <= SMALL else []:

            @pl.when(zed == k)
            def _(k=k):
                for target in range(k):
                    offer((0, 0, k ^ target)).start()

        for peer in reversed(peers):
            if peer[2] == 0 or size_c > SMALL:
                pl.when(within(peer))(offer(peer).start)

        @pl.when(core == 0)
        def _():
            pl.semaphore_wait(ready.at[0], 1)

        relay(0)
        for peer in peers:
            if (peer[2] == 0 and not diagonal(peer)) or size_c > SMALL:
                pl.when(outer(peer))(functools.partial(answered, peer))
        if cross:

            @pl.when(spot == 0)
            def _():
                for peer in peers:
                    if peer[2] == 0 and not diagonal(peer):
                        answer((1, 1, 0), at_step(*peer))

        if size_c > SMALL:
            for t in line[1:]:
                arrive(t)
            return
        for k in line:

            @pl.when(zed == k)
            def _(k=k):
                near = sorted(line[1:], key=lambda t: (abs((k ^ t) - k), k ^ t))
                away = [(0, 0, t) for t in near if k ^ t > k]
                for peer in away:
                    answered(peer)
                for peer in peers:
                    if diagonal(peer):
                        pl.when(beyond(peer))(functools.partial(answered, peer))
                for t in near:
                    arrive(t)

    own = [
        pltpu.make_async_copy(pos, raw_pos, local_sem.at[0]),
        pltpu.make_async_copy(mass, raw_mass, local_sem.at[1]),
        pltpu.make_async_copy(blocks, raw_pair.at[0], local_sem.at[2]),
        pltpu.make_async_copy(halos, raw_pair.at[1], local_sem.at[3]),
        pltpu.make_async_copy(cen, cen_out, local_sem.at[4]),
        pltpu.make_async_copy(rad, rad_out, local_sem.at[5]),
    ]
    barrier = pltpu.get_barrier_semaphore()

    def greet(device):
        pl.semaphore_signal(barrier, inc=1, device_id=device, device_id_type=MESH)

    for one in own:
        one.start()
    for peer in peers:
        pl.when(greeted(peer))(functools.partial(greet, at_step(*peer)))
    pl.when(core == 0)(functools.partial(greet, sibling))
    lower = zed + spot + core
    if cross:
        lower = lower - jnp.where(spot == 2, 1, 0)

    @pl.when(lower > 0)
    def _():
        pl.semaphore_wait(barrier, lower)

    for peer in peers:
        pl.when(within(peer))(functools.partial(answer, peer, at_step(*peer)))
    pl.when(core == 1)(functools.partial(answer, (0, 0, 0), sibling))
    for one in own:
        one.wait()
    mine = place_of[0]
    for b in range(count):
        part = raw_pos[:, b * BLOCK : (b + 1) * BLOCK]
        for i in range(3):
            data[mine, i * count + b : i * count + b + 1, :] = part[i : i + 1]
    data[mine, 3 * count : 4 * count, :] = raw_mass[...]
    groups_of = lax.broadcasted_iota(jnp.int32, (1, 128), 1) // share
    for i in range(2):
        values = raw_pair[i].astype(jnp.float32)
        turned = {0: values}
        for z in line:
            for row in range(asks):
                total = jnp.zeros((1, 128), jnp.float32)
                for part in range(128 // share):
                    start = ((row * (128 // share) + part) * size_c + z) * share
                    turn = (part * share - start) % 128
                    if turn not in turned:
                        turned[turn] = pltpu.roll(values, turn, 1)
                    piece = turned[turn][start // 128 : start // 128 + 1]
                    total = jnp.where(groups_of == part, piece, total)
                asking[z, i * asks + row : i * asks + row + 1, :] = total
    data[mine, pl.ds(body_rows, 2 * asks), :] = asking[zed]
    state[...] = jnp.zeros_like(state)
    terms[...] = jnp.zeros_like(terms)
    state[0:3, :] = cen_out[...]
    state[3:4, :] = rad_out[...]
    state[4:5, :] = lax.broadcasted_iota(jnp.int32, (1, halo_dev), 1).astype(jnp.float32)
    state[5:6, :] = jnp.ones((1, halo_dev), jnp.float32)
    begin()

    lane0 = lax.rem(mx * share, 128) + lax.rem(my, 2) * slots
    lanes = lax.broadcasted_iota(jnp.int32, (GROUP, halo_dev), 1).astype(jnp.float32)
    spots = lax.broadcasted_iota(jnp.int32, (GROUP, GROUP * count), 1).astype(jnp.float32)
    place = lax.broadcasted_iota(jnp.int32, (GROUP, 128), 0).astype(jnp.float32)
    shift = lax.rem(128 - lane0, 128)

    def prepare(g):
        lo = g * GROUP * slots
        if not isinstance(g, int):
            lo = pl.multiple_of(lo, GROUP * slots)

        def taken(i):
            at = body_rows + i * asks + row_me
            part = data[pl.ds(g * GROUP, GROUP), pl.ds(at, 1), :].reshape(GROUP, 128)
            return pltpu.roll(part, shift, 1)

        rows = taken(1)
        want = taken(0) + place * float(count)
        for j in range(0, slots, 2):
            start = lo + j * GROUP
            for values, iota, out in ((rows, lanes, onehot), (want, spots, pick)):
                pair = [
                    jnp.where(values[:, i : i + 1] == iota, 1.0, 0.0) for i in (j, j + 1)
                ]
                both = jnp.concatenate(pair, axis=0).astype(jnp.bfloat16)
                out[pl.ds(start, 2 * GROUP), :] = both
            for i in (j, j + 1):
                column = jnp.broadcast_to(rows[:, i : i + 1], (GROUP, GROUP * slots))
                cols[pl.ds(lo + i * GROUP, GROUP), :] = column
        asked[:, pl.ds(lo, GROUP * slots)] = join3(
            lax.dot_general(
                split3(state[...]), onehot[pl.ds(lo, GROUP * slots), :], (((1,), (1,)), ((), ())),
                preferred_element_type=jnp.float32,
            )
        )

    def relate(g):
        def block(h):
            return pl.ds(h * width, width)

        def meet(down, across):
            key = asked[4:5, block(across)]
            key = jnp.where(asked[5:6, block(across)] > 0.5, key, -2.0)
            equal = cols[block(down), :] == key
            same[block(down), block(across)] = jnp.where(equal, 1.0, 0.0).astype(jnp.bfloat16)

        for h in range(g + 1):
            meet(g, h)
        for h in range(g):
            meet(h, g)

    width = GROUP * slots
    kept = (SHELLS // 2 - 1, SHELLS, SHELLS + 1, SHELLS + 2, SHELLS + 3)

    def evaluate(g, keep=False):
        lo = pl.multiple_of(g * width, width)
        mine = asked[0:4, pl.ds(lo, width)]
        cx, cy, cz, radius = (mine[i : i + 1] for i in range(4))
        scale = (SHELLS / 2.0) / jnp.where(radius > 0.0, radius, 1.0)

        def fold(value):
            return jnp.sum(value.reshape(CHUNK // 8, 8, width), axis=0)

        def chunk(c, acc):
            at = pl.ds(pl.multiple_of(c * CHUNK, CHUNK), CHUNK)
            ox = points[g, 0, at] - cx
            oy = points[g, 1, at] - cy
            oz = points[g, 2, at] - cz
            m = points[g, 3, at]
            u = jnp.sqrt(ox * ox + oy * oy + oz * oz) * scale
            ramp = m * (0.5 - u)
            out = []
            for k in range(SHELLS + 1):
                out.append(acc[k] + fold(jnp.maximum(ramp, 0.0)))
                ramp = ramp + m
            inner = m * jnp.clip(SHELLS / 2.0 - u, 0.0, 1.0)
            out.append(acc[SHELLS + 1] + fold(inner))
            for i, o in enumerate((ox, oy, oz)):
                out.append(acc[SHELLS + 2 + i] + fold(o * inner))
            return tuple(out)

        zero = jnp.zeros((8, width), jnp.float32)
        acc = lax.fori_loop(0, BLOCK // CHUNK, chunk, (zero,) * (SHELLS + 5), unroll=True)
        acc = [acc[k + 1] - acc[k] - acc[0] for k in range(SHELLS)] + list(acc[SHELLS + 1 :])
        for k in range(SHELLS + 4):
            value = jnp.sum(acc[k], axis=0, keepdims=True)
            terms[k : k + 1, pl.ds(lo, width)] = value
            if keep and k in kept:
                at = KEEP + kept.index(k)
                terms[at : at + 1, pl.ds(lo, width)] = value

    def choose(g):
        chosen = pick[pl.ds(pl.multiple_of(g * width, width), width), :]
        for i in range(4):
            flat = data[pl.ds(g * GROUP, GROUP), i * count : (i + 1) * count, :]
            flat = flat.reshape(GROUP * count, BLOCK).T
            points[g, i] = join3(
                lax.dot_general(
                    split3(flat), chosen, (((1,), (1,)), ((), ())),
                    preferred_element_type=jnp.float32,
                )
            )

    def again(g, _):
        evaluate(g)
        return 0

    def grown(radius, enclosed):
        ratio = (1.0 + enclosed) / (1.0 + radius * radius * radius)
        return radius * jnp.exp(jnp.log(ratio) * (1.0 / 3.0))

    def gather_sums(values, table):
        return join3(
            lax.dot_general(
                split3(values), table, (((1,), (0,)), ((), ())),
                preferred_element_type=jnp.float32,
            )
        )

    def move_slots():
        part = gather_sums(terms[SHELLS : 2 * SHELLS], same[...])
        enclosed = part[KEEP - SHELLS : KEEP - SHELLS + 1]
        total = jnp.maximum(part[0:1], 1.0)
        asked[3:4, :] = grown(asked[3:4, :], enclosed)
        asked[0:3, :] = asked[0:3, :] + part[1:4] / total

    def plane_of(p1):
        for p3, p2 in reversed(plane):
            arrive(label(p3, p2, p1))

    def finish(g):
        late = sum(rank[i][3] >= half for i in range(g * GROUP, (g + 1) * GROUP))
        if late:
            several(late, half - 1 + g).wait_recv()
        prepare(g)
        relate(g)
        choose(g)
        evaluate(g, True)

    def closer(k):
        return sorted(line[1:], key=lambda t: (abs((k ^ t) - k), k ^ t))

    plane_of(0)
    finish(0)
    if size_c <= SMALL:
        for k in line:

            @pl.when(zed == k)
            def _(k=k):
                for i, p1 in enumerate(closer(k)):
                    plane_of(p1)
                    if k == 0 and i == 0:
                        finish(1)

        pl.when(zed > 0)(functools.partial(finish, 1))
    else:
        for p1 in line[1:]:
            plane_of(p1)
        finish(1)
    for g in range(2, groups):
        finish(g)
    move_slots()
    lax.fori_loop(0, groups, again, 0)
    sums = gather_sums(terms[...], onehot[...])
    center, radius = state[0:3, :], state[3:4, :]
    for first in (KEEP, None):
        if first is None:
            enclosed, inner = sums[SHELLS // 2 - 1 : SHELLS // 2], sums[SHELLS : SHELLS + 4]
        else:
            enclosed, inner = sums[first : first + 1], sums[first + 1 : first + 5]
        radius = grown(radius, enclosed)
        center = center + inner[1:4] / jnp.maximum(inner[0:1], 1.0)
    cen_out[...] = center
    rad_out[...] = radius
    prof_out[...] = sums[:SHELLS]
    several(n - 1, 0).wait_send()


def hand(a, b, c, x, y, z, sem):
    copies = [
        pltpu.make_async_copy(source, target, sem.at[i])
        for i, (source, target) in enumerate(((a, x), (b, y), (c, z)))
    ]
    for copy in copies:
        copy.start()
    for copy in copies:
        copy.wait()


def body(positions, masses, centers, radii, pair_block, pair_halo):
    ndx = lax.axis_size("dx")
    ndy = lax.axis_size("dy")
    n = ndx * ndy
    halo_dev = radii.shape[0]
    count = masses.shape[0] // BLOCK
    slots = pair_halo.shape[0] // n
    total = n * slots
    groups = n // GROUP
    any_ref = pl.BlockSpec(memory_space=pl.ANY)
    vmem = pl.BlockSpec(memory_space=pltpu.VMEM)
    f32 = jnp.float32
    dma = pltpu.SemaphoreType.DMA
    out = pl.pallas_call(
        functools.partial(kernel, (ndx, ndy, slots, count)),
        out_shape=(
            pltpu.VMEM((3, halo_dev), f32),
            pltpu.VMEM((1, halo_dev), f32),
            pltpu.VMEM((SHELLS, halo_dev), f32),
        ),
        in_specs=[any_ref] * 6,
        out_specs=(vmem,) * 3,
        scratch_shapes=[
            pltpu.VMEM((3, count * BLOCK), f32),
            pltpu.VMEM((count, BLOCK), f32),
            pltpu.VMEM((2, total // 128, 128), jnp.int32),
            pltpu.VMEM((ndy // 2, ndx * slots // 32, BLOCK), f32),
            pltpu.VMEM((n, 4 * count + ndx * slots // 32, BLOCK), f32),
            pltpu.VMEM((total, GROUP * count), jnp.bfloat16),
            pltpu.VMEM((groups, 4, BLOCK, GROUP * slots), f32),
            pltpu.VMEM((total, halo_dev), jnp.bfloat16),
            pltpu.VMEM((total, GROUP * slots), f32),
            pltpu.VMEM((total, total), jnp.bfloat16),
            pltpu.VMEM((ROWS, total), f32),
            pltpu.VMEM((16, halo_dev), f32),
            pltpu.VMEM((16, total), f32),
            dma((6,)),
            dma((1,)),
            dma((n // 2 - 1 + groups,)),
            pltpu.SemaphoreType.REGULAR((ndx + ndy // 2,)),
        ],
        compiler_params=pltpu.CompilerParams(collective_id=0, has_side_effects=True),
    )(
        positions,
        masses.reshape(count, BLOCK),
        centers,
        radii.reshape(1, halo_dev),
        pair_block.reshape(total // 128, 128),
        pair_halo.reshape(total // 128, 128),
    )
    out = [pltpu.with_memory_space_constraint(x, pltpu.VMEM) for x in out]
    out = pl.pallas_call(
        hand,
        out_shape=tuple(jax.ShapeDtypeStruct(x.shape, f32) for x in out),
        in_specs=[vmem] * 3,
        out_specs=(any_ref,) * 3,
        scratch_shapes=[dma((3,))],
    )(*out)
    return out[0], out[1].reshape(halo_dev), out[2]


def solution(mesh):
    flat = P(("dx", "dy"))
    rows = P(None, ("dx", "dy"))
    in_specs = (rows, flat, rows, flat, flat, flat)
    out_specs = (rows, flat, rows)
    return jax.shard_map(body, mesh=mesh, in_specs=in_specs, out_specs=out_specs, check_vma=False)
```
